64 devices in a mesh: rep: 4 (over x, y), fsdp: 16 (over z, core).
Axes of the slice: x: 2, y: 2, z: 8, core: 2. Of those that a mesh axis runs over, the one named last changes fastest.
The devices are a block of a 4x4x8 slice.
Arguments:
- act_in: bfloat16 [12, 32768, 768], P(None, ('rep', 'fsdp')), parts along dimension 1
- cot_out: bfloat16 [12, 32768, 768], P(None, ('rep', 'fsdp')), parts along dimension 1
- lengths: int32 [12, 64], P(None, ('rep', 'fsdp')), parts along dimension 1
- w_in: bfloat16 [1, 768, 3072], P(None, 'fsdp')
- w_out: bfloat16 [1, 3072, 768], P(None, 'fsdp')
Outputs:
- output 1: float32 [1, 3072, 3072], P(None, ('rep', 'fsdp')), parts along dimension 1
- output 2: float32 [1, 12288, 768], P(None, ('rep', 'fsdp')), parts along dimension 1
There are 4 independent parts. The reference program is written for one: setup_inputs(seed, part) draws one part's arguments, and reference() takes and returns one part's arrays. A program takes and returns all parts, laid end to end along the dimension named above; an argument that names none is the same for every part.
All inputs are finite; a program needn't handle non-finite values.
Results may differ from the reference program's by a relative error of at most 0.00938265.
Values are sent between devices in bfloat16 or wider.
A program may use at most 768 MiB of HBM per device.

```python
import math
import jax
import jax.numpy as jnp
from jax import lax

MICRO_BATCHES = 12
TOKENS_DEV = 512
GROUP_DEVS = 16
D_MODEL = 768
D_FF = 3072
LAYERS = 1

GROUP_TOKENS = TOKENS_DEV * GROUP_DEVS
MIN_LEN = TOKENS_DEV // 8
COT_SCALE = (MICRO_BATCHES * GROUP_TOKENS) ** -0.5
SQRT_HALF = math.sqrt(0.5)
INV_SQRT_TAU = 1.0 / math.sqrt(2.0 * math.pi)


def gelu_fwd(pre_act):
    return 0.5 * pre_act * (1.0 + lax.erf(pre_act * SQRT_HALF))


def gelu_grad(pre_act):
    return 0.5 * (1.0 + lax.erf(pre_act * SQRT_HALF)) + pre_act * jnp.exp(-0.5 * pre_act * pre_act) * INV_SQRT_TAU


def draw_lengths(key):
    k_draw, k_long, k_short = jax.random.split(key, 3)
    slot_count = MICRO_BATCHES * GROUP_DEVS
    len_draw = jax.random.randint(k_draw, (slot_count,), MIN_LEN, TOKENS_DEV + 1)
    long_pos = jax.random.randint(k_long, (), 0, slot_count)
    short_pos = (long_pos + jax.random.randint(k_short, (), 1, slot_count)) % slot_count
    slot_idx = jnp.arange(slot_count)
    len_draw = jnp.where(slot_idx == long_pos, TOKENS_DEV, len_draw)
    len_draw = jnp.where(slot_idx == short_pos, MIN_LEN, len_draw)
    return len_draw.reshape(MICRO_BATCHES, GROUP_DEVS).astype(jnp.int32)


def setup_inputs(seed: int = 0, part: int = 0) -> dict:
    base_key = jax.random.key(seed)
    part_key = jax.random.fold_in(base_key, part)
    k_act, k_cot, k_len = jax.random.split(part_key, 3)
    k_up, k_down = jax.random.split(jax.random.key(seed + 1), 2)
    act_in = jax.random.normal(k_act, (MICRO_BATCHES, GROUP_TOKENS, D_MODEL), jnp.float32)
    cot_out = jax.random.normal(k_cot, (MICRO_BATCHES, GROUP_TOKENS, D_MODEL), jnp.float32) * COT_SCALE
    w_in = jax.random.normal(k_up, (LAYERS, D_MODEL, D_FF), jnp.float32) * D_MODEL ** -0.5
    w_out = jax.random.normal(k_down, (LAYERS, D_FF, D_MODEL), jnp.float32) * D_FF ** -0.5
    return {
        'act_in': act_in.astype(jnp.bfloat16),
        'cot_out': cot_out.astype(jnp.bfloat16),
        'lengths': draw_lengths(k_len),
        'w_in': w_in.astype(jnp.bfloat16),
        'w_out': w_out.astype(jnp.bfloat16),
    }


def reference(act_in, cot_out, lengths, w_in, w_out):
    block_count = MICRO_BATCHES * GROUP_DEVS
    act_blocks = act_in.reshape(block_count, TOKENS_DEV, D_MODEL)
    cot_blocks = cot_out.reshape(block_count, TOKENS_DEV, D_MODEL)
    len_blocks = lengths.reshape(block_count)
    tok_pos = jnp.arange(TOKENS_DEV)

    def fwd_layer(hidden, weights):
        w_up, w_down = weights
        pre_act = jnp.dot(hidden, w_up, preferred_element_type=jnp.float32).astype(jnp.bfloat16)
        post_act = gelu_fwd(pre_act.astype(jnp.float32)).astype(jnp.bfloat16)
        hidden_next = (hidden.astype(jnp.float32) + jnp.dot(post_act, w_down, preferred_element_type=jnp.float32)).astype(jnp.bfloat16)
        return hidden_next, (hidden, pre_act, post_act)

    def bwd_layer(cot_cur, items):
        w_up, w_down, hidden, pre_act, post_act = items
        grad_down = jnp.dot(post_act.T, cot_cur, preferred_element_type=jnp.float32)
        d_act = jnp.dot(cot_cur, w_down.T, preferred_element_type=jnp.float32)
        d_pre = (d_act * gelu_grad(pre_act.astype(jnp.float32))).astype(jnp.bfloat16)
        grad_up = jnp.dot(hidden.T, d_pre, preferred_element_type=jnp.float32)
        cot_prev = (cot_cur.astype(jnp.float32) + jnp.dot(d_pre, w_up.T, preferred_element_type=jnp.float32)).astype(jnp.bfloat16)
        return cot_prev, (grad_up, grad_down)

    def one_block(carry, block_in):
        acc_in, acc_out = carry
        act_blk, cot_blk, len_blk = block_in
        cot_kept = jnp.where((tok_pos < len_blk)[:, None], cot_blk, jnp.zeros_like(cot_blk))
        hidden_last, saved = lax.scan(fwd_layer, act_blk, (w_in, w_out))
        cot_first, grads = lax.scan(bwd_layer, cot_kept, (w_in, w_out) + saved, reverse=True)
        return (acc_in + grads[0], acc_out + grads[1]), None

    init_acc = (jnp.zeros((LAYERS, D_MODEL, D_FF), jnp.float32), jnp.zeros((LAYERS, D_FF, D_MODEL), jnp.float32))
    totals, unused_out = lax.scan(one_block, init_acc, (act_blocks, cot_blocks, len_blocks))
    return totals[0], totals[1]
```

```python
import functools
import math
import jax
import jax.numpy as jnp
from jax import lax
from jax.experimental import pallas as pl
from jax.experimental.pallas import tpu as pltpu
from jax.sharding import PartitionSpec as P

SQRT_HALF = math.sqrt(0.5)
INV_SQRT_TAU = 1.0 / math.sqrt(2.0 * math.pi)
F32 = jnp.float32
BF16 = jnp.bfloat16
MESH = pl.DeviceIdType.MESH
NT_DIMS = (((1,), (1,)), ((), ()))

SLICE = 256
LANES = 2
HEAD = 3
LONG, SHORT = 4, 3


def gelu_pair(pre_act):
    cdf = 0.5 * (1.0 + lax.erf(pre_act * SQRT_HALF))
    return pre_act * cdf, cdf + pre_act * jnp.exp(-0.5 * pre_act * pre_act) * INV_SQRT_TAU


def dot_nt(left, right):
    return lax.dot_general(left, right, NT_DIMS, preferred_element_type=F32)


def dot_nn(left, right):
    return jnp.dot(left, right, preferred_element_type=F32)


def step_kernel(cfg, act_hbm, cot_hbm, len_smem, wts_hbm, out_hbm,
                act_t, cot, stage, wts, up_t, down, acc, post_s, dpre_s,
                peer, ring_in, ring_out, fin,
                load_sem, agl_s, agl_r, ags_s, ags_r, agx_s, agx_r,
                ex_s, ex_r, rl_s, rl_r, rs_s, rs_r, fin_s, fin_r):
    n_slice, n_dev, micro, toks, width, tiles = cfg
    n_chip = n_dev // 2
    per_dev = SLICE_OF(cfg) // n_dev
    n_blk = width // SLICE_OF(cfg)
    rows_dev = width // n_dev
    chunk = 2 * per_dev
    dev = lax.axis_index('fsdp')
    chip = dev // 2
    core = dev % 2
    sgn = 1 - 2 * core

    def at_chip(off):
        return (chip + sgn * off + 2 * n_chip) % n_chip

    nxt = at_chip(1) * 2 + core
    prv = at_chip(-1) * 2 + core
    sib = chip * 2 + 1 - core

    def remote(src, dst, send, recv, target):
        return pltpu.make_async_remote_copy(src_ref=src, dst_ref=dst, send_sem=send, recv_sem=recv,
                                            device_id={'fsdp': target}, device_id_type=MESH)

    barrier = pltpu.get_barrier_semaphore()
    for other in (nxt, prv, sib):
        pl.semaphore_signal(barrier, inc=1, device_id={'fsdp': other}, device_id_type=MESH)

    own_load = pltpu.make_async_copy(wts_hbm, wts.at[:, dev], load_sem.at[2 * micro])
    own_load.start()

    def act_load(k):
        return pltpu.make_async_copy(act_hbm.at[k], stage.at[k % 4], load_sem.at[k])

    def cot_load(k):
        return pltpu.make_async_copy(cot_hbm.at[k], cot.at[k // LANES, pl.ds((k % LANES) * toks, toks)],
                                     load_sem.at[micro + k])

    for k in range(4):
        act_load(k).start()
        cot_load(k).start()
    own_load.wait()
    pl.semaphore_wait(barrier, 3)

    def piece(q, off):
        return wts.at[q, at_chip(off) * 2 + core]

    def ag_long(q, t):
        ref = piece(q, 1 - t)
        return remote(ref, ref, agl_s.at[q, t - 1], agl_r.at[q, t - 1], nxt)

    def ag_short(q, t):
        ref = piece(q, t - 1)
        return remote(ref, ref, ags_s.at[q, t - 1], ags_r.at[q, t - 1], prv)

    def ag_sib(q, idx, off):
        ref = piece(q, off)
        return remote(ref, ref, agx_s.at[q, idx], agx_r.at[q, idx], sib)

    def ag_first(q):
        ag_long(q, 1).start()
        ag_short(q, 1).start()
        ag_sib(q, 0, 0).start()

    def ag_mid(q, t):
        ag_long(q, t - 1).wait_recv()
        ag_long(q, t).start()
        ag_sib(q, t - 1, 1 - t).start()
        ag_short(q, t - 1).wait_recv()

        @pl.when(t <= SHORT)
        def _():
            ag_short(q, t).start()
        ag_sib(q, LONG + t - 1, t - 1).start()

    def ag_last(q):
        ag_long(q, LONG).wait_recv()
        ag_sib(q, LONG, -LONG).start()

    def ag_finish(q):
        for idx in range(LONG + SHORT + 1):
            ag_sib(q, idx, 0).wait_recv()
        for idx in range(LONG + SHORT + 1):
            ag_sib(q, idx, 0).wait_send()
        for t in range(1, LONG + 1):
            ag_long(q, t).wait_send()
        for t in range(1, SHORT + 1):
            ag_short(q, t).wait_send()

    def load_tile(k):
        act_load(k).wait()
        act_t[k // LANES, :, (k % LANES) * toks:(k % LANES + 1) * toks] = stage[k % 4].T
        cot_load(k).wait()
        row = lax.broadcasted_iota(jnp.int32, (toks, 1), 0)
        rows = pl.ds((k % LANES) * toks, toks)
        val = cot[k // LANES, rows, :]
        cot[k // LANES, rows, :] = jnp.where(row < len_smem[k, 0], val, jnp.zeros_like(val))
        if k + 4 < micro:
            act_load(k + 4).start()
            cot_load(k + 4).start()

    for q in range(HEAD):
        ag_first(q)
    per_tick = micro // LONG
    for t in range(2, LONG + 2):
        for k in range((t - 2) * per_tick, (t - 1) * per_tick):
            load_tile(k)
        for q in range(HEAD):
            if t <= LONG:
                ag_mid(q, t)
            else:
                ag_last(q)

    def exchange(q):
        return remote(acc.at[q % 4, 1 - core], peer.at[q % 3], ex_s.at[q % 3], ex_r.at[q % 3], sib)

    def send_long(q, t):
        return remote(ring_out.at[q % 3, t - 1], ring_in.at[q % 3, t - 1],
                      rl_s.at[q % 3, t - 1], rl_r.at[q % 3, t - 1], nxt)

    def send_short(q, t):
        return remote(ring_out.at[q % 3, LONG + t - 1], ring_in.at[q % 3, LONG + t - 1],
                      rs_s.at[q % 3, t - 1], rs_r.at[q % 3, t - 1], prv)

    def own_sum(q, off):
        rows = pl.ds(pl.multiple_of(at_chip(off) * chunk, chunk), chunk)
        return acc[q % 4, core, rows, :] + peer[q % 3, rows, :]

    def send_fin(q):
        return remote(ring_out.at[q % 3, LONG + SHORT, pl.ds(pl.multiple_of((1 - core) * per_dev, per_dev), per_dev)],
                      fin.at[core, q], fin_s.at[q], fin_r.at[q], sib)

    def rs_exchange(q):
        @pl.when(q >= 3)
        def _():
            send_fin(q - 3).wait_recv()
        exchange(q).start()

    def rs_round(q, t):
        if t == 1:
            exchange(q).wait_recv()
        val = own_sum(q, 5 - t)
        if t > 1:
            send_long(q, t - 1).wait_recv()
            val = val + ring_in[q % 3, t - 2]
        ring_out[q % 3, t - 1] = val
        if t <= SHORT:
            val = own_sum(q, t - 4)
            if t > 1:
                send_short(q, t - 1).wait_recv()
                val = val + ring_in[q % 3, LONG + t - 2]
            ring_out[q % 3, LONG + t - 1] = val
        send_long(q, t).start()
        if t <= SHORT:
            send_short(q, t).start()

    def rs_final(q):
        val = own_sum(q, 0)
        send_long(q, LONG).wait_recv()
        send_short(q, SHORT).wait_recv()
        val = val + ring_in[q % 3, LONG - 1] + ring_in[q % 3, LONG + SHORT - 1]
        ring_out[q % 3, LONG + SHORT] = val
        send_fin(q).start()
        mine = pl.ds(pl.multiple_of(core * per_dev, per_dev), per_dev)
        fin[core, q] = ring_out[q % 3, LONG + SHORT, mine]
        exchange(q).wait_send()
        for t in range(1, LONG + 1):
            send_long(q, t).wait_send()
        for t in range(1, SHORT + 1):
            send_short(q, t).wait_send()
        send_fin(q).wait_send()

    def guarded(q, fn):
        @pl.when(jnp.logical_and(q >= 0, q < n_slice))
        def _():
            fn(q)

    def comm(s, t):
        @pl.when(t == 0)
        def _():
            guarded(s - 1, rs_exchange)

        @pl.when(t == 1 % tiles)
        def _():
            guarded(s - 1, lambda q: rs_round(q, 1))

        @pl.when(t == 2 % tiles)
        def _():
            guarded(s - 2, lambda q: rs_round(q, 3))
            guarded(s - 3, rs_final)

        @pl.when(t == 4 % tiles)
        def _():
            guarded(s - 1, lambda q: rs_round(q, 2))

        @pl.when(t == 5 % tiles)
        def _():
            guarded(s - 2, lambda q: rs_round(q, 4))

    def gather(n):
        half = n // 2
        q2 = 2 * HEAD + (half - 4) // 4
        t2 = (half + 4) % 4 + 1

        @pl.when(n == 0)
        def _():
            for q in range(HEAD, 2 * HEAD):
                ag_first(q)

        @pl.when(jnp.logical_and(half >= 1, half <= 3))
        def _():
            for q in range(HEAD, 2 * HEAD):
                ag_mid(q, half + 1)

        @pl.when(half == 4)
        def _():
            for q in range(HEAD, 2 * HEAD):
                ag_last(q)

        @pl.when(jnp.logical_and(half >= 4, q2 < n_slice))
        def _():
            @pl.when(t2 == 1)
            def _():
                ag_first(q2)

            @pl.when(t2 > 1)
            def _():
                ag_mid(q2, t2)

        @pl.when(jnp.logical_and(jnp.logical_and(half >= 8, t2 == 1), q2 <= n_slice))
        def _():
            ag_last(q2 - 1)

    def main(n, carry):
        s = n // tiles
        t = n % tiles

        @pl.when(t == 0)
        def _():
            ag_finish(s)
            up_t[...] = wts[s, :, 0:rows_dev, :].reshape(width, n_dev * per_dev).T
            for b in range(n_blk):
                lo = rows_dev + b * per_dev
                down[:, b * n_dev * per_dev:(b + 1) * n_dev * per_dev] = (
                    wts[s, :, lo:lo + per_dev, :].reshape(n_dev * per_dev, n_dev * per_dev))
            acc[s % 4] = jnp.zeros((2, n_dev * per_dev, width), F32)

        pre = dot_nn(up_t[...], act_t[t]).astype(BF16).astype(F32)
        post, slope = gelu_pair(pre)
        d_act = dot_nt(down[...], cot[t])
        post_s[...] = post.astype(BF16)
        dpre_s[...] = (d_act * slope).astype(BF16)
        acc[s % 4, 0] += dot_nn(post_s[...], cot[t])
        g_in = dot_nt(act_t[t], dpre_s[...])
        for d in range(n_dev):
            for b in range(n_blk):
                lo = d * rows_dev + b * per_dev
                acc[s % 4, 1, d * per_dev:(d + 1) * per_dev, b * n_dev * per_dev:(b + 1) * n_dev * per_dev] += (
                    g_in[lo:lo + per_dev])

        @pl.when(n % 2 == 0)
        def _():
            gather(n)
        comm(s, t)
        return carry

    lax.fori_loop(0, n_slice * tiles, main, 0)

    def tail(n, carry):
        comm(n // tiles, n % tiles)
        return carry

    lax.fori_loop(n_slice * tiles, (n_slice + 2) * tiles + 3, tail, 0)
    for q in range(n_slice - 3, n_slice):
        send_fin(q).wait_recv()
    done = pltpu.make_async_copy(fin, out_hbm, load_sem.at[0])
    done.start()
    done.wait()


def SLICE_OF(cfg):
    return min(SLICE, cfg[4] // 3)


def run_step(n_dev, act, cot, lengths, w_in, w_out):
    micro, toks, width = act.shape
    hidden = w_in.shape[1]
    sl = min(SLICE, width // 3)
    n_slice, per_dev, n_blk, rows_dev = hidden // sl, sl // n_dev, width // sl, width // n_dev
    tiles = micro // LANES
    cfg = (n_slice, n_dev, micro, toks, width, tiles)
    up = w_in.reshape(rows_dev, n_dev, n_slice, per_dev).transpose(2, 0, 1, 3).reshape(n_slice, rows_dev, sl)
    down = w_out.reshape(n_slice, per_dev, n_blk, sl).transpose(0, 2, 1, 3).reshape(n_slice, rows_dev, sl)
    wts = jnp.concatenate([up, down], axis=1)
    hbm = pl.BlockSpec(memory_space=pl.ANY)
    dma = pltpu.SemaphoreType.DMA
    chunk = 2 * per_dev
    tok = toks * LANES
    out = pl.pallas_call(
        functools.partial(step_kernel, cfg),
        name='mlp_grads',
        out_shape=jax.ShapeDtypeStruct((2, n_slice, per_dev, width), F32),
        in_specs=[hbm, hbm, pl.BlockSpec(memory_space=pltpu.SMEM), hbm],
        out_specs=hbm,
        scratch_shapes=[
            pltpu.VMEM((tiles, width, tok), BF16),
            pltpu.VMEM((tiles, tok, width), BF16),
            pltpu.VMEM((4, toks, width), BF16),
            pltpu.VMEM((n_slice, n_dev, 2 * rows_dev, sl), BF16),
            pltpu.VMEM((sl, width), BF16),
            pltpu.VMEM((sl, width), BF16),
            pltpu.VMEM((4, 2, sl, width), F32),
            pltpu.VMEM((sl, tok), BF16),
            pltpu.VMEM((sl, tok), BF16),
            pltpu.VMEM((3, sl, width), F32),
            pltpu.VMEM((3, LONG + SHORT, chunk, width), F32),
            pltpu.VMEM((3, LONG + SHORT + 1, chunk, width), F32),
            pltpu.VMEM((2, n_slice, per_dev, width), F32),
            dma((2 * micro + 1,)),
            dma((n_slice, LONG)), dma((n_slice, LONG)), dma((n_slice, SHORT)), dma((n_slice, SHORT)),
            dma((n_slice, LONG + SHORT + 1)), dma((n_slice, LONG + SHORT + 1)),
            dma((3,)), dma((3,)), dma((3, LONG)), dma((3, LONG)), dma((3, SHORT)), dma((3, SHORT)),
            dma((n_slice,)), dma((n_slice,)),
        ],
        compiler_params=pltpu.CompilerParams(collective_id=0, has_side_effects=True, vmem_limit_bytes=62 * 2 ** 20),
    )(act, cot, lengths, wts)
    grad_out = out[0].reshape(n_slice * per_dev, width)
    grad_in = out[1].reshape(n_slice, per_dev, n_blk, n_dev, per_dev).transpose(2, 1, 3, 0, 4)
    return grad_in.reshape(rows_dev, hidden), grad_out


def solution(mesh):
    n_dev = mesh.shape['fsdp']
    shard_spec = P(None, ('rep', 'fsdp'), None)
    len_spec = P(None, ('rep', 'fsdp'))
    weight_spec = P(None, 'fsdp', None)

    def local_step(act_in, cot_out, lengths, w_in, w_out):
        grad_in, grad_out = run_step(n_dev, act_in, cot_out, lengths, w_in[0], w_out[0])
        return grad_in[None], grad_out[None]

    return jax.shard_map(local_step, mesh=mesh, in_specs=(shard_spec, shard_spec, len_spec, weight_spec, weight_spec),
                         out_specs=(shard_spec, shard_spec), check_vma=False)
```

```python
import functools
import math
import jax
import jax.numpy as jnp
from jax import lax
from jax.experimental import pallas as pl
from jax.experimental.pallas import tpu as pltpu
from jax.sharding import PartitionSpec as P

SQRT_HALF = math.sqrt(0.5)
INV_SQRT_TAU = 1.0 / math.sqrt(2.0 * math.pi)
F32 = jnp.float32
BF16 = jnp.bfloat16
MESH = pl.DeviceIdType.MESH
NT_DIMS = (((1,), (1,)), ((), ()))

SLICE = 256
LANES = 2
HEAD = 3
LONG, SHORT = 4, 3


def gelu_pair(pre_act):
    cdf = 0.5 * (1.0 + lax.erf(pre_act * SQRT_HALF))
    return pre_act * cdf, cdf + pre_act * jnp.exp(-0.5 * pre_act * pre_act) * INV_SQRT_TAU


def dot_nt(left, right):
    return lax.dot_general(left, right, NT_DIMS, preferred_element_type=F32)


def dot_nn(left, right):
    return jnp.dot(left, right, preferred_element_type=F32)


def step_kernel(cfg, act_hbm, cot_hbm, len_smem, up_hbm, down_hbm, gin_hbm, gout_hbm,
                act_t, cot, stage, wts, up_t, down, acc, post_s, dpre_s,
                peer, ring_in, ring_out, fin, gin,
                load_sem, agl_s, agl_r, ags_s, ags_r, agx_s, agx_r,
                ex_s, ex_r, rl_s, rl_r, rs_s, rs_r, fin_s, fin_r):
    n_slice, n_dev, micro, toks, width, tiles = cfg
    n_chip = n_dev // 2
    per_dev = SLICE_OF(cfg) // n_dev
    n_blk = width // SLICE_OF(cfg)
    rows_dev = width // n_dev
    chunk = 2 * per_dev
    dev = lax.axis_index('fsdp')
    chip = dev // 2
    core = dev % 2
    sgn = 1 - 2 * core

    def at_chip(off):
        return (chip + sgn * off + 2 * n_chip) % n_chip

    nxt = at_chip(1) * 2 + core
    prv = at_chip(-1) * 2 + core
    sib = chip * 2 + 1 - core

    def remote(src, dst, send, recv, target):
        return pltpu.make_async_remote_copy(src_ref=src, dst_ref=dst, send_sem=send, recv_sem=recv,
                                            device_id={'fsdp': target}, device_id_type=MESH)

    barrier = pltpu.get_barrier_semaphore()
    for other in (nxt, prv, sib):
        pl.semaphore_signal(barrier, inc=1, device_id={'fsdp': other}, device_id_type=MESH)

    sl = n_dev * per_dev
    own_loads = [pltpu.make_async_copy(up_hbm, wts.at[:, dev, pl.ds(0, rows_dev)], load_sem.at[2 * micro])]
    for b in range(n_blk):
        own_loads.append(pltpu.make_async_copy(down_hbm.at[:, :, pl.ds(b * sl, sl)],
                                               wts.at[:, dev, pl.ds(rows_dev + b * per_dev, per_dev)],
                                               load_sem.at[2 * micro + 1 + b]))
    for copy in own_loads:
        copy.start()

    def act_load(k):
        return pltpu.make_async_copy(act_hbm.at[k], stage.at[k % 4], load_sem.at[k])

    def cot_load(k):
        return pltpu.make_async_copy(cot_hbm.at[k], cot.at[k // LANES, pl.ds((k % LANES) * toks, toks)],
                                     load_sem.at[micro + k])

    for k in range(4):
        act_load(k).start()
        cot_load(k).start()
    for copy in own_loads:
        copy.wait()
    with jax.named_scope('bar'):
        pl.semaphore_wait(barrier, 3)

    def piece(q, off):
        return wts.at[q, at_chip(off) * 2 + core]

    def ag_long(q, t):
        ref = piece(q, 1 - t)
        return remote(ref, ref, agl_s.at[q, t - 1], agl_r.at[q, t - 1], nxt)

    def ag_short(q, t):
        ref = piece(q, t - 1)
        return remote(ref, ref, ags_s.at[q, t - 1], ags_r.at[q, t - 1], prv)

    def ag_sib(q, idx, off):
        ref = piece(q, off)
        return remote(ref, ref, agx_s.at[q, idx], agx_r.at[q, idx], sib)

    def ag_first(q):
        ag_long(q, 1).start()
        ag_short(q, 1).start()
        ag_sib(q, 0, 0).start()

    def ag_mid(q, t):
        ag_long(q, t - 1).wait_recv()
        ag_long(q, t).start()
        ag_sib(q, t - 1, 1 - t).start()
        ag_short(q, t - 1).wait_recv()

        if t <= SHORT:
            ag_short(q, t).start()
        ag_sib(q, LONG + t - 1, t - 1).start()

    def ag_last(q):
        ag_long(q, LONG).wait_recv()
        ag_sib(q, LONG, -LONG).start()

    def ag_finish(q):
        for idx in range(LONG + SHORT + 1):
            ag_sib(q, idx, 0).wait_recv()
        for idx in range(LONG + SHORT + 1):
            ag_sib(q, idx, 0).wait_send()
        for t in range(1, LONG + 1):
            ag_long(q, t).wait_send()
        for t in range(1, SHORT + 1):
            ag_short(q, t).wait_send()

    def load_tile(k):
        act_load(k).wait()
        act_t[k // LANES, :, (k % LANES) * toks:(k % LANES + 1) * toks] = stage[k % 4].T
        cot_load(k).wait()
        row = lax.broadcasted_iota(jnp.int32, (toks, 1), 0)
        rows = pl.ds((k % LANES) * toks, toks)
        val = cot[k // LANES, rows, :]
        cot[k // LANES, rows, :] = jnp.where(row < len_smem[k], val, jnp.zeros_like(val))
        if k + 4 < micro:
            act_load(k + 4).start()
            cot_load(k + 4).start()

    def ag_step(q, t):
        if t == 1:
            ag_first(q)
        elif t <= LONG:
            ag_mid(q, t)
        else:
            ag_last(q)

    ag_step(0, 1)
    per_tick = micro // LONG
    for tick in range(2, LONG + 2):
        with jax.named_scope(f'load{tick}'):
            for k in range((tick - 2) * per_tick, (tick - 1) * per_tick):
                load_tile(k)
        with jax.named_scope(f'head{tick}'):
            for q in range(HEAD):
                if tick - q >= 1:
                    ag_step(q, tick - q)

    def exchange(q):
        return remote(acc.at[q % 4, 1 - core], peer.at[q % 3], ex_s.at[q % 3], ex_r.at[q % 3], sib)

    def send_long(q, t):
        return remote(ring_out.at[q % 3, t - 1], ring_in.at[q % 3, t - 1],
                      rl_s.at[q % 3, t - 1], rl_r.at[q % 3, t - 1], nxt)

    def send_short(q, t):
        return remote(ring_out.at[q % 3, LONG + t - 1], ring_in.at[q % 3, LONG + t - 1],
                      rs_s.at[q % 3, t - 1], rs_r.at[q % 3, t - 1], prv)

    def own_sum(q, off):
        rows = pl.ds(pl.multiple_of(at_chip(off) * chunk, chunk), chunk)
        return acc[q % 4, core, rows, :] + peer[q % 3, rows, :]

    def send_fin(q):
        return remote(ring_out.at[q % 3, LONG + SHORT, pl.ds(pl.multiple_of((1 - core) * per_dev, per_dev), per_dev)],
                      fin.at[core, q], fin_s.at[q], fin_r.at[q], sib)

    def rs_exchange(q):
        @pl.when(q >= 3)
        def _():
            send_fin(q - 3).wait_recv()
            send_fin(q - 3).wait_send()
        exchange(q).start()

    def rs_round(q, t):
        if t == 1:
            exchange(q).wait_recv()
        val = own_sum(q, 5 - t)
        if t > 1:
            send_long(q, t - 1).wait_recv()
            val = val + ring_in[q % 3, t - 2]
        ring_out[q % 3, t - 1] = val
        if t <= SHORT:
            val = own_sum(q, t - 4)
            if t > 1:
                send_short(q, t - 1).wait_recv()
                val = val + ring_in[q % 3, LONG + t - 2]
            ring_out[q % 3, LONG + t - 1] = val
        send_long(q, t).start()
        if t <= SHORT:
            send_short(q, t).start()

    def rs_final(q):
        val = own_sum(q, 0)
        send_long(q, LONG).wait_recv()
        send_short(q, SHORT).wait_recv()
        val = val + ring_in[q % 3, LONG - 1] + ring_in[q % 3, LONG + SHORT - 1]
        ring_out[q % 3, LONG + SHORT] = val
        send_fin(q).start()
        mine = pl.ds(pl.multiple_of(core * per_dev, per_dev), per_dev)
        fin[core, q] = ring_out[q % 3, LONG + SHORT, mine]
        exchange(q).wait_send()
        for t in range(1, LONG + 1):
            send_long(q, t).wait_send()
        for t in range(1, SHORT + 1):
            send_short(q, t).wait_send()

    spread = 7 if tiles <= 5 else 8
    plan = [('exch', 0, rs_exchange)]
    for t, off in ((1, 1), (2, 4), (3, spread), (4, spread + 3)):
        plan.append((f'r{t}', off, functools.partial(rs_round, t=t)))
    plan.append(('fin', spread + 6, rs_final))

    def comm(n):
        for name, off, fn in plan:
            back = n - off

            @pl.when(jnp.logical_and(back >= tiles, back % tiles == 0))
            def _(name=name, fn=fn, back=back):
                with jax.named_scope(name):
                    q = back // tiles - 1

                    @pl.when(q < n_slice)
                    def _():
                        fn(q)

    def gather(n):
        for tick in range(LONG + 2, LONG + 1 + HEAD):
            @pl.when(n == 2 * (tick - LONG - 2))
            def _(tick=tick):
                for q in range(HEAD):
                    if tick - q <= LONG + 1:
                        ag_step(q, tick - q)

        for t in range(1, LONG + 2):
            @pl.when(n == 2 * (t - 1))
            def _(t=t):
                for q in range(HEAD, 2 * HEAD):
                    ag_step(q, t)

            off = n - 2 * LONG - 2 * (t - 1)
            q = 2 * HEAD + off // (tiles + 2)

            @pl.when(jnp.logical_and(off >= 0, jnp.logical_and(off % (tiles + 2) == 0, q < n_slice)))
            def _(t=t, q=q):
                ag_step(q, t)

    def main(n, carry):
        s = n // tiles
        t = n % tiles

        @pl.when(t == 0)
        def _():
            with jax.named_scope('agfin'):
                ag_finish(s)
            up_t[...] = wts[s, :, 0:rows_dev, :].reshape(width, n_dev * per_dev).T
            for b in range(n_blk):
                lo = rows_dev + b * per_dev
                down[:, b * n_dev * per_dev:(b + 1) * n_dev * per_dev] = (
                    wts[s, :, lo:lo + per_dev, :].reshape(n_dev * per_dev, n_dev * per_dev))
            acc[s % 4] = jnp.zeros((2, n_dev * per_dev, width), F32)

        pre = dot_nn(up_t[...], act_t[t]).astype(BF16).astype(F32)
        post, slope = gelu_pair(pre)
        d_act = dot_nt(down[...], cot[t])
        post_s[...] = post.astype(BF16)
        dpre_s[...] = (d_act * slope).astype(BF16)
        acc[s % 4, 0] += dot_nn(post_s[...], cot[t])
        g_in = dot_nt(act_t[t], dpre_s[...])
        for d in range(n_dev):
            for b in range(n_blk):
                lo = d * rows_dev + b * per_dev
                acc[s % 4, 1, d * per_dev:(d + 1) * per_dev, b * n_dev * per_dev:(b + 1) * n_dev * per_dev] += (
                    g_in[lo:lo + per_dev])

        with jax.named_scope('gath'):
            gather(n)
        comm(n)
        return carry

    lax.fori_loop(0, n_slice * tiles, main, 0)

    def tail(n, carry):
        comm(n)
        return carry

    lax.fori_loop(n_slice * tiles, n_slice * tiles + spread + 7, tail, 0)
    for q in range(n_slice - 3, n_slice):
        send_fin(q).wait_recv()
        send_fin(q).wait_send()
    done_out = pltpu.make_async_copy(fin.at[0], gout_hbm, load_sem.at[0])
    done_out.start()
    with jax.named_scope('perm'):
        run = n_slice * per_dev
        group = 128 // per_dev if n_dev * run % 128 == 0 and 128 % per_dev == 0 else 1
        for b in range(n_blk):
            for c in range(n_dev * n_slice // group):
                parts = []
                for k in range(group):
                    d, q = divmod(c * group + k, n_slice)
                    parts.append(fin[1, q, :, b * sl + d * per_dev:b * sl + (d + 1) * per_dev])
                gin[b * per_dev:(b + 1) * per_dev, c * group * per_dev:(c + 1) * group * per_dev] = (
                    jnp.concatenate(parts, axis=1))
    done_in = pltpu.make_async_copy(gin, gin_hbm, load_sem.at[1])
    done_in.start()
    done_out.wait()
    done_in.wait()


def SLICE_OF(cfg):
    return min(SLICE, cfg[4] // 3)


def run_step(n_dev, act, cot, lengths, w_in, w_out):
    micro, toks, width = act.shape
    hidden = w_in.shape[1]
    sl = min(SLICE, width // 3)
    n_slice, per_dev, n_blk, rows_dev = hidden // sl, sl // n_dev, width // sl, width // n_dev
    tiles = micro // LANES
    cfg = (n_slice, n_dev, micro, toks, width, tiles)
    up = w_in.reshape(rows_dev, n_dev, n_slice, per_dev).transpose(2, 0, 1, 3).reshape(n_slice, rows_dev, sl)
    down = w_out.reshape(n_slice, per_dev, width)
    hbm = pl.BlockSpec(memory_space=pl.ANY)
    dma = pltpu.SemaphoreType.DMA
    chunk = 2 * per_dev
    tok = toks * LANES
    out = pl.pallas_call(
        functools.partial(step_kernel, cfg),
        name='mlp_grads',
        out_shape=(jax.ShapeDtypeStruct((rows_dev, hidden), F32), jax.ShapeDtypeStruct((n_slice, per_dev, width), F32)),
        in_specs=[hbm, hbm, pl.BlockSpec(memory_space=pltpu.SMEM), hbm, hbm],
        out_specs=(hbm, hbm),
        scratch_shapes=[
            pltpu.VMEM((tiles, width, tok), BF16),
            pltpu.VMEM((tiles, tok, width), BF16),
            pltpu.VMEM((4, toks, width), BF16),
            pltpu.VMEM((n_slice, n_dev, 2 * rows_dev, sl), BF16),
            pltpu.VMEM((sl, width), BF16),
            pltpu.VMEM((sl, width), BF16),
            pltpu.VMEM((4, 2, sl, width), F32),
            pltpu.VMEM((sl, tok), BF16),
            pltpu.VMEM((sl, tok), BF16),
            pltpu.VMEM((3, sl, width), F32),
            pltpu.VMEM((3, LONG + SHORT, chunk, width), F32),
            pltpu.VMEM((3, LONG + SHORT + 1, chunk, width), F32),
            pltpu.VMEM((2, n_slice, per_dev, width), F32),
            pltpu.VMEM((rows_dev, hidden), F32),
            dma((2 * micro + 1 + n_blk,)),
            dma((n_slice, LONG)), dma((n_slice, LONG)), dma((n_slice, SHORT)), dma((n_slice, SHORT)),
            dma((n_slice, LONG + SHORT + 1)), dma((n_slice, LONG + SHORT + 1)),
            dma((3,)), dma((3,)), dma((3, LONG)), dma((3, LONG)), dma((3, SHORT)), dma((3, SHORT)),
            dma((n_slice,)), dma((n_slice,)),
        ],
        compiler_params=pltpu.CompilerParams(collective_id=0, has_side_effects=True, vmem_limit_bytes=62 * 2 ** 20),
    )(act, cot, lengths.reshape(micro), up, down)
    return out[0], out[1].reshape(n_slice * per_dev, width)


def solution(mesh):
    n_dev = mesh.shape['fsdp']
    shard_spec = P(None, ('rep', 'fsdp'), None)
    len_spec = P(None, ('rep', 'fsdp'))
    weight_spec = P(None, 'fsdp', None)

    def local_step(act_in, cot_out, lengths, w_in, w_out):
        grad_in, grad_out = run_step(n_dev, act_in, cot_out, lengths, w_in[0], w_out[0])
        return grad_in[None], grad_out[None]

    return jax.shard_map(local_step, mesh=mesh, in_specs=(shard_spec, shard_spec, len_spec, weight_spec, weight_spec),
                         out_specs=(shard_spec, shard_spec), check_vma=False)
```

```python
import functools
import math
import jax
import jax.numpy as jnp
from jax import lax
from jax.experimental import pallas as pl
from jax.experimental.pallas import tpu as pltpu
from jax.sharding import PartitionSpec as P

SQRT_HALF = math.sqrt(0.5)
INV_SQRT_TAU = 1.0 / math.sqrt(2.0 * math.pi)
F32 = jnp.float32
BF16 = jnp.bfloat16
MESH = pl.DeviceIdType.MESH
NT_DIMS = (((1,), (1,)), ((), ()))

SLICE = 256
LANES = 2
HEAD = 3
LONG, SHORT = 4, 3


def gelu_pair(pre_act):
    cdf = 0.5 * (1.0 + lax.erf(pre_act * SQRT_HALF))
    return pre_act * cdf, cdf + pre_act * jnp.exp(-0.5 * pre_act * pre_act) * INV_SQRT_TAU


def dot_nt(left, right):
    return lax.dot_general(left, right, NT_DIMS, preferred_element_type=F32)


def dot_nn(left, right):
    return jnp.dot(left, right, preferred_element_type=F32)


def step_kernel(cfg, act_hbm, cot_hbm, len_smem, up_hbm, down_hbm, fin_hbm,
                act_t, cot, stage, wts, up_t, down, acc, post_s, dpre_s,
                peer, ring_in, ring_out, fin,
                load_sem, agl_s, agl_r, ags_s, ags_r, agx_s, agx_r,
                ex_s, ex_r, rl_s, rl_r, rs_s, rs_r, fin_s, fin_r):
    n_slice, n_dev, micro, toks, width, tiles = cfg
    n_chip = n_dev // 2
    per_dev = SLICE_OF(cfg) // n_dev
    n_blk = width // SLICE_OF(cfg)
    rows_dev = width // n_dev
    chunk = 2 * per_dev
    dev = lax.axis_index('fsdp')
    chip = dev // 2
    core = dev % 2
    sgn = 1 - 2 * core

    def at_chip(off):
        return (chip + sgn * off + 2 * n_chip) % n_chip

    nxt = at_chip(1) * 2 + core
    prv = at_chip(-1) * 2 + core
    sib = chip * 2 + 1 - core

    def remote(src, dst, send, recv, target):
        return pltpu.make_async_remote_copy(src_ref=src, dst_ref=dst, send_sem=send, recv_sem=recv,
                                            device_id={'fsdp': target}, device_id_type=MESH)

    barrier = pltpu.get_barrier_semaphore()
    for other in (nxt, prv, sib):
        pl.semaphore_signal(barrier, inc=1, device_id={'fsdp': other}, device_id_type=MESH)

    sl = n_dev * per_dev
    own_loads = [pltpu.make_async_copy(up_hbm, wts.at[:, dev, pl.ds(0, rows_dev)], load_sem.at[2 * micro])]
    for b in range(n_blk):
        own_loads.append(pltpu.make_async_copy(down_hbm.at[:, :, pl.ds(b * sl, sl)],
                                               wts.at[:, dev, pl.ds(rows_dev + b * per_dev, per_dev)],
                                               load_sem.at[2 * micro + 1 + b]))
    for copy in own_loads:
        copy.start()

    def act_load(k):
        return pltpu.make_async_copy(act_hbm.at[k], stage.at[k % 4], load_sem.at[k])

    def cot_load(k):
        return pltpu.make_async_copy(cot_hbm.at[k], cot.at[k // LANES, pl.ds((k % LANES) * toks, toks)],
                                     load_sem.at[micro + k])

    for k in range(4):
        act_load(k).start()
        cot_load(k).start()
    for copy in own_loads:
        copy.wait()
    pl.semaphore_wait(barrier, 3)

    def piece(q, off):
        return wts.at[q, at_chip(off) * 2 + core]

    def ag_long(q, t):
        ref = piece(q, 1 - t)
        return remote(ref, ref, agl_s.at[q, t - 1], agl_r.at[q, t - 1], nxt)

    def ag_short(q, t):
        ref = piece(q, t - 1)
        return remote(ref, ref, ags_s.at[q, t - 1], ags_r.at[q, t - 1], prv)

    def ag_sib(q, idx, off):
        ref = piece(q, off)
        return remote(ref, ref, agx_s.at[q, idx], agx_r.at[q, idx], sib)

    def ag_first(q):
        ag_long(q, 1).start()
        ag_short(q, 1).start()
        ag_sib(q, 0, 0).start()

    def ag_mid(q, t):
        ag_long(q, t - 1).wait_recv()
        ag_long(q, t).start()
        ag_sib(q, t - 1, 1 - t).start()
        ag_short(q, t - 1).wait_recv()

        if t <= SHORT:
            ag_short(q, t).start()
        ag_sib(q, LONG + t - 1, t - 1).start()

    def ag_last(q):
        ag_long(q, LONG).wait_recv()
        ag_sib(q, LONG, -LONG).start()

    def ag_finish(q):
        for idx in range(LONG + SHORT + 1):
            ag_sib(q, idx, 0).wait_recv()
        for idx in range(LONG + SHORT + 1):
            ag_sib(q, idx, 0).wait_send()
        for t in range(1, LONG + 1):
            ag_long(q, t).wait_send()
        for t in range(1, SHORT + 1):
            ag_short(q, t).wait_send()

    def load_tile(k):
        act_load(k).wait()
        act_t[k // LANES, :, (k % LANES) * toks:(k % LANES + 1) * toks] = stage[k % 4].T
        cot_load(k).wait()
        row = lax.broadcasted_iota(jnp.int32, (toks, 1), 0)
        rows = pl.ds((k % LANES) * toks, toks)
        val = cot[k // LANES, rows, :]
        cot[k // LANES, rows, :] = jnp.where(row < len_smem[k], val, jnp.zeros_like(val))
        if k + 4 < micro:
            act_load(k + 4).start()
            cot_load(k + 4).start()

    def ag_step(q, t):
        if t == 1:
            ag_first(q)
        elif t <= LONG:
            ag_mid(q, t)
        else:
            ag_last(q)

    ag_step(0, 1)
    per_tick = micro // LONG
    for tick in range(2, LONG + 2):
        for k in range((tick - 2) * per_tick, (tick - 1) * per_tick):
            load_tile(k)
        for q in range(HEAD):
            if tick - q >= 1:
                ag_step(q, tick - q)

    need = (4, -3, 3, -2, 2, -1, 1, 0)

    def rows_at(off):
        return pl.ds(pl.multiple_of(at_chip(off) * chunk, chunk), chunk)

    def half_at(off, h):
        return pl.ds(pl.multiple_of(at_chip(off) * chunk + h * per_dev, per_dev), per_dev)

    def exchange(q, off):
        i = need.index(off)
        return remote(acc.at[q % 4, 1 - core, rows_at(-off)], peer.at[q % 3, rows_at(-off)],
                      ex_s.at[q % 3, i], ex_r.at[q % 3, i], sib)

    def send_long(q, t, h):
        return remote(ring_out.at[q % 3, t - 1, h], ring_in.at[q % 3, t - 1, h],
                      rl_s.at[q % 3, t - 1, h], rl_r.at[q % 3, t - 1, h], nxt)

    def send_short(q, t, h):
        return remote(ring_out.at[q % 3, LONG + t - 1, h], ring_in.at[q % 3, LONG + t - 1, h],
                      rs_s.at[q % 3, t - 1, h], rs_r.at[q % 3, t - 1, h], prv)

    def own_sum(q, off, h):
        rows = half_at(off, h)
        return acc[q % 4, core, rows, :] + peer[q % 3, rows, :]

    def send_fin(q):
        return remote(ring_out.at[q % 3, LONG + SHORT, 1 - core], fin.at[core, q], fin_s.at[q], fin_r.at[q], sib)

    def rs_exchange(q):
        def settle():
            send_fin(q - 3).wait_recv()
            send_fin(q - 3).wait_send()
        if isinstance(q, int):
            if q >= 3:
                settle()
        else:
            pl.when(q >= 3)(settle)
        for off in need:
            exchange(q, off).start()

    def rs_round(q, t):
        exchange(q, 5 - t).wait_recv()
        if t <= SHORT:
            exchange(q, t - 4).wait_recv()
        for h in (core, 1 - core):
            val = own_sum(q, 5 - t, h)
            if t > 1:
                send_long(q, t - 1, h).wait_recv()
                val = val + ring_in[q % 3, t - 2, h]
            ring_out[q % 3, t - 1, h] = val
            if t <= SHORT:
                val = own_sum(q, t - 4, h)
                if t > 1:
                    send_short(q, t - 1, h).wait_recv()
                    val = val + ring_in[q % 3, LONG + t - 2, h]
                ring_out[q % 3, LONG + t - 1, h] = val
            send_long(q, t, h).start()
            if t <= SHORT:
                send_short(q, t, h).start()

    def rs_final(q):
        exchange(q, 0).wait_recv()
        for h in (core, 1 - core):
            val = own_sum(q, 0, h)
            send_long(q, LONG, h).wait_recv()
            send_short(q, SHORT, h).wait_recv()
            ring_out[q % 3, LONG + SHORT, h] = val + ring_in[q % 3, LONG - 1, h] + ring_in[q % 3, LONG + SHORT - 1, h]
        send_fin(q).start()
        fin[core, q] = ring_out[q % 3, LONG + SHORT, core]
        for off in need:
            exchange(q, off).wait_send()
        for h in range(2):
            for t in range(1, LONG + 1):
                send_long(q, t, h).wait_send()
            for t in range(1, SHORT + 1):
                send_short(q, t, h).wait_send()

    plan = [(0, rs_exchange)]
    for t, off in ((1, 1), (2, 4), (3, 8), (4, 11)):
        plan.append((off, functools.partial(rs_round, t=t)))
    plan.append((14, rs_final))

    def gather(s, t):
        if t in (0, 2):
            @pl.when(s == 0)
            def _():
                for q in range(HEAD):
                    if LONG + 2 + t // 2 - q <= LONG + 1:
                        ag_step(q, LONG + 2 + t // 2 - q)
        if t in (0, 2, 4):
            @pl.when(s == 0)
            def _():
                for q in range(HEAD, 2 * HEAD):
                    ag_step(q, t // 2 + 1)
        if t in (0, 2):
            @pl.when(s == 1)
            def _():
                for q in range(HEAD, 2 * HEAD):
                    ag_step(q, t // 2 + LONG)
        if t in (1, 3, 5):
            q = s + 2 * HEAD - 1

            @pl.when(jnp.logical_and(s >= 1, q < n_slice))
            def _():
                ag_step(q, t // 2 + 1)
        if t in (1, 3):
            q_old = s + 2 * HEAD - 2

            @pl.when(jnp.logical_and(s >= 2, q_old < n_slice))
            def _():
                ag_step(q_old, t // 2 + LONG)

    def main(s, carry):
        ag_finish(s)
        up_t[...] = wts[s, :, 0:rows_dev, :].reshape(width, sl).T
        for b in range(n_blk):
            lo = rows_dev + b * per_dev
            down[:, b * sl:(b + 1) * sl] = wts[s, :, lo:lo + per_dev, :].reshape(sl, sl)
        acc[s % 4] = jnp.zeros((2, sl, width), F32)
        for t in range(tiles):
            pre = dot_nn(up_t[...], act_t[t]).astype(BF16).astype(F32)
            post, slope = gelu_pair(pre)
            d_act = dot_nt(down[...], cot[t])
            post_s[...] = post.astype(BF16)
            dpre_s[...] = (d_act * slope).astype(BF16)
            acc[s % 4, 0] += dot_nn(post_s[...], cot[t])
            g_in = dot_nt(act_t[t], dpre_s[...])
            for d in range(n_dev):
                for b in range(n_blk):
                    lo = d * rows_dev + b * per_dev
                    acc[s % 4, 1, d * per_dev:(d + 1) * per_dev, b * sl:(b + 1) * sl] += g_in[lo:lo + per_dev]
            gather(s, t)
            for off, fn in plan:
                if off % tiles == t:
                    q = s - 1 - off // tiles

                    @pl.when(q >= 0)
                    def _(q=q, fn=fn):
                        fn(q)
        return carry

    lax.fori_loop(0, n_slice, main, 0)
    for n in range(n_slice * tiles, n_slice * tiles + 15):
        for off, fn in plan:
            q = (n - off) // tiles - 1
            if (n - off) % tiles == 0 and q < n_slice:
                fn(q)
    for q in range(n_slice - 3, n_slice):
        send_fin(q).wait_recv()
        send_fin(q).wait_send()
    done = pltpu.make_async_copy(fin, fin_hbm, load_sem.at[0])
    done.start()
    done.wait()


def order_kernel(dims, fin_hbm, gin_hbm, gout_hbm, fin_out, fin_in, gin, sem):
    n_slice, n_dev, per_dev, n_blk, sl = dims
    get_in = pltpu.make_async_copy(fin_hbm.at[1], fin_in, sem.at[0])
    get_out = pltpu.make_async_copy(fin_hbm.at[0], fin_out, sem.at[1])
    put_out = pltpu.make_async_copy(fin_out, gout_hbm, sem.at[2])
    get_in.start()
    get_out.start()
    get_in.wait()
    group = 128 // per_dev if n_dev * n_slice * per_dev % 128 == 0 and 128 % per_dev == 0 else 1
    for b in range(n_blk):
        for c in range(n_dev * n_slice // group):
            parts = []
            for k in range(group):
                d, q = divmod(c * group + k, n_slice)
                parts.append(fin_in[q, :, b * sl + d * per_dev:b * sl + (d + 1) * per_dev])
            gin[b * per_dev:(b + 1) * per_dev, c * group * per_dev:(c + 1) * group * per_dev] = jnp.concatenate(parts, axis=1)
        if b == 0:
            get_out.wait()
            put_out.start()
    put_in = pltpu.make_async_copy(gin, gin_hbm, sem.at[3])
    put_in.start()
    put_out.wait()
    put_in.wait()


def SLICE_OF(cfg):
    return min(SLICE, cfg[4] // 3)


def run_step(n_dev, act, cot, lengths, w_in, w_out):
    micro, toks, width = act.shape
    hidden = w_in.shape[1]
    sl = min(SLICE, width // 3)
    n_slice, per_dev, n_blk, rows_dev = hidden // sl, sl // n_dev, width // sl, width // n_dev
    tiles = micro // LANES
    cfg = (n_slice, n_dev, micro, toks, width, tiles)
    up = w_in.reshape(rows_dev, n_dev, n_slice, per_dev).transpose(2, 0, 1, 3).reshape(n_slice, rows_dev, sl)
    down = w_out.reshape(n_slice, per_dev, width)
    hbm = pl.BlockSpec(memory_space=pl.ANY)
    dma = pltpu.SemaphoreType.DMA
    tok = toks * LANES
    out = pl.pallas_call(
        functools.partial(step_kernel, cfg),
        name='mlp_grads',
        out_shape=jax.ShapeDtypeStruct((2, n_slice, per_dev, width), F32),
        in_specs=[hbm, hbm, pl.BlockSpec(memory_space=pltpu.SMEM), hbm, hbm],
        out_specs=hbm,
        scratch_shapes=[
            pltpu.VMEM((tiles, width, tok), BF16),
            pltpu.VMEM((tiles, tok, width), BF16),
            pltpu.VMEM((4, toks, width), BF16),
            pltpu.VMEM((n_slice, n_dev, 2 * rows_dev, sl), BF16),
            pltpu.VMEM((sl, width), BF16),
            pltpu.VMEM((sl, width), BF16),
            pltpu.VMEM((4, 2, sl, width), F32),
            pltpu.VMEM((sl, tok), BF16),
            pltpu.VMEM((sl, tok), BF16),
            pltpu.VMEM((3, sl, width), F32),
            pltpu.VMEM((3, LONG + SHORT, 2, per_dev, width), F32),
            pltpu.VMEM((3, LONG + SHORT + 1, 2, per_dev, width), F32),
            pltpu.VMEM((2, n_slice, per_dev, width), F32),
            dma((2 * micro + 1 + n_blk,)),
            dma((n_slice, LONG)), dma((n_slice, LONG)), dma((n_slice, SHORT)), dma((n_slice, SHORT)),
            dma((n_slice, LONG + SHORT + 1)), dma((n_slice, LONG + SHORT + 1)),
            dma((3, 8)), dma((3, 8)), dma((3, LONG, 2)), dma((3, LONG, 2)), dma((3, SHORT, 2)), dma((3, SHORT, 2)),
            dma((n_slice,)), dma((n_slice,)),
        ],
        compiler_params=pltpu.CompilerParams(collective_id=0, has_side_effects=True, vmem_limit_bytes=62 * 2 ** 20),
    )(act, cot, lengths.reshape(micro), up, down)
    grad_in, grad_out = pl.pallas_call(
        functools.partial(order_kernel, (n_slice, n_dev, per_dev, n_blk, sl)),
        name='order_columns',
        out_shape=(jax.ShapeDtypeStruct((rows_dev, hidden), F32), jax.ShapeDtypeStruct((n_slice, per_dev, width), F32)),
        in_specs=[hbm],
        out_specs=(hbm, hbm),
        scratch_shapes=[
            pltpu.VMEM((n_slice, per_dev, width), F32),
            pltpu.VMEM((n_slice, per_dev, width), F32),
            pltpu.VMEM((rows_dev, hidden), F32),
            dma((4,)),
        ],
    )(out)
    return grad_in, grad_out.reshape(n_slice * per_dev, width)


def solution(mesh):
    n_dev = mesh.shape['fsdp']
    shard_spec = P(None, ('rep', 'fsdp'), None)
    len_spec = P(None, ('rep', 'fsdp'))
    weight_spec = P(None, 'fsdp', None)

    def local_step(act_in, cot_out, lengths, w_in, w_out):
        grad_in, grad_out = run_step(n_dev, act_in, cot_out, lengths, w_in[0], w_out[0])
        return grad_in[None], grad_out[None]

    return jax.shard_map(local_step, mesh=mesh, in_specs=(shard_spec, shard_spec, len_spec, weight_spec, weight_spec),
                         out_specs=(shard_spec, shard_spec), check_vma=False)
```
